32 devices in a mesh: ctx: 8 (over y, x, core), tp: 4 (over z).
Axes of the slice: x: 2, y: 2, z: 4, core: 2. Of those that a mesh axis runs over, the one named last changes fastest.
Arguments:
- queries: bfloat16 [1024, 16384], P('ctx', 'tp'), may hold values from -110 to 110
- key_value_cache: bfloat16 [2, 5120, 1024], P(None, 'ctx', 'tp'), may hold values from -9 to 9
- cache_lengths: int32 [8], P('ctx'), may hold values from 64 to 512, as said below
- token_order: int32 [1024], P('ctx'), may hold values from 0 to 1023, each once
- out_weight: bfloat16 [16384, 16384], P('tp', 'ctx'), may hold values from -0.046875 to 0.046875
Outputs:
- output: bfloat16 [1024, 16384], P('tp', 'ctx')
The draws below stay inside these ranges and needn't reach their ends.
Inputs may be any that keep to these rules, and one draw needn't show every extreme that they name: `cache_lengths`: one shard's cache is full in every draw. `token_order`: each number of 0 to 1023 stands once.
All inputs are finite; a program needn't handle non-finite values.
Results may differ from the reference program's by a relative error of at most 0.04.
Values may be sent and summed in bfloat16 or wider, within the bound.
A program may use at most 64 MiB of HBM per device.

```python
import math
import jax
import jax.numpy as jnp
from jax import lax

D = 16384
QUERY_HEADS = 128
KEY_VALUE_HEADS = 8
HEAD_SIZE = 128
TOKENS_PER_SHARD = 128
CACHE_DEV = 512
SHARD_ROWS = 640
NEW_TOKENS = 1024
KEY_VALUE_ROWS = 5120
N_CTX = 8


def shared_tensors(key):
    key_entries, value_entries, key_queries = jax.random.split(jax.random.fold_in(key, 7), 3)
    key_matrix = jnp.clip(jax.random.normal(key_entries, (KEY_VALUE_ROWS, KEY_VALUE_HEADS * HEAD_SIZE), jnp.float32), -4.5, 4.5)
    value_matrix = jnp.clip(jax.random.normal(value_entries, (KEY_VALUE_ROWS, KEY_VALUE_HEADS * HEAD_SIZE), jnp.float32), -4.5, 4.5)
    queries = 3.0 * jnp.clip(jax.random.normal(key_queries, (NEW_TOKENS, QUERY_HEADS * HEAD_SIZE), jnp.float32), -6.0, 6.0)
    return (queries, key_matrix, value_matrix)


def draw_queries(key, part):
    queries, key_matrix, value_matrix = shared_tensors(key)
    return queries.astype(jnp.bfloat16)


def draw_key_value_cache(key, part):
    queries, key_matrix, value_matrix = shared_tensors(key)
    return jnp.stack([key_matrix, value_matrix]).astype(jnp.bfloat16)


def draw_cache_lengths(key, part):
    first, second_part = jax.random.split(jax.random.fold_in(key, 11))
    shards = KEY_VALUE_ROWS // SHARD_ROWS
    lengths = jax.random.randint(first, (shards,), max(2, CACHE_DEV // 8), CACHE_DEV // 2 + 1)
    fullest = jax.random.randint(second_part, (), 0, shards)
    return jnp.where(jnp.arange(shards) == fullest, CACHE_DEV, lengths).astype(jnp.int32)


def level_of(stream_key, extent, pieces, smallest, high):
    def one(position, parts):
        heights = jax.random.uniform(jax.random.fold_in(jax.random.fold_in(stream_key, 6), position), (parts,), jnp.float32, smallest / len(pieces), high / len(pieces))
        return jnp.repeat(jnp.exp(heights), extent[position] // parts).reshape((-1,) + (1,) * (len(extent) - position - 1))

    gain = one(*pieces[0])
    for cut in pieces[1:]:
        gain = gain * one(*cut)
    return gain


def noise(own_key, shape, scale, limit, pieces=(), held_as=jnp.bfloat16):
    loudness = level_of(own_key, shape, pieces, -0.22, 0.18) if pieces else 1.0
    array = jax.random.normal(own_key, shape, jnp.float32) * scale * loudness
    return jnp.minimum(jnp.maximum(array, -limit), limit).astype(held_as)


def setup_inputs(seed: int = 0) -> dict:
    key_list = jax.random.split(jax.random.key(seed), 6)
    queries = draw_queries(jax.random.fold_in(key_list[5], 71), 0)
    key_value_cache = draw_key_value_cache(jax.random.fold_in(key_list[5], 71), 0)
    cache_lengths = draw_cache_lengths(jax.random.fold_in(key_list[5], 71), 0)
    token_order = jax.random.permutation(key_list[3], NEW_TOKENS).astype(jnp.int32)
    out_weight = noise(key_list[4], (QUERY_HEADS * HEAD_SIZE, D), (QUERY_HEADS * HEAD_SIZE) ** -0.5, 0.046875, ((0, 4), (1, 8)))
    return dict(queries=queries, key_value_cache=key_value_cache, cache_lengths=cache_lengths, token_order=token_order, out_weight=out_weight)


def reference(queries, key_value_cache, cache_lengths, token_order, out_weight):
    group_index = QUERY_HEADS // KEY_VALUE_HEADS
    scale = 1.0 / math.sqrt(HEAD_SIZE)
    within = jnp.arange(SHARD_ROWS, dtype=jnp.int32)
    cache_valid = (within[None, :] < cache_lengths[:, None]) & (within[None, :] < CACHE_DEV)
    latest = jnp.full((N_CTX, CACHE_DEV), NEW_TOKENS, jnp.int32)
    key_order = jnp.concatenate([latest, token_order.reshape(N_CTX, TOKENS_PER_SHARD).astype(jnp.int32)], axis=1)
    cache_valid = cache_valid.reshape(KEY_VALUE_ROWS)
    key_order = key_order.reshape(KEY_VALUE_ROWS)
    key_matrix = jnp.transpose(key_value_cache[0].astype(jnp.float32).reshape(KEY_VALUE_ROWS, KEY_VALUE_HEADS, HEAD_SIZE), (1, 0, 2))
    value_matrix = jnp.transpose(key_value_cache[1].astype(jnp.float32).reshape(KEY_VALUE_ROWS, KEY_VALUE_HEADS, HEAD_SIZE), (1, 0, 2))
    block_list = queries.reshape(N_CTX, TOKENS_PER_SHARD, KEY_VALUE_HEADS, group_index, HEAD_SIZE)
    orders = token_order.reshape(N_CTX, TOKENS_PER_SHARD).astype(jnp.int32)

    def one_block(pair):
        block_slice, order = pair
        allowed = cache_valid[None, :] | (key_order[None, :] <= order[:, None])

        def one_head(triple):
            heads, head_keys, head_values = triple
            scores = jnp.einsum('tgd,nd->gtn', heads.astype(jnp.float32), head_keys) * scale
            scores = jnp.where(allowed[None], scores, -jnp.inf)
            peak = lax.optimization_barrier(jnp.max(scores, axis=-1, keepdims=True))
            raised = jnp.exp(scores - peak)
            total = lax.optimization_barrier(jnp.sum(raised, axis=-1, keepdims=True))
            weights = lax.optimization_barrier(raised.astype(jnp.bfloat16)).astype(jnp.float32)
            return jnp.einsum('gtn,nd->gtd', weights, head_values) / total
        mixed = lax.map(one_head, (jnp.transpose(block_slice, (1, 0, 2, 3)), key_matrix, value_matrix))
        return jnp.transpose(mixed, (2, 0, 1, 3)).reshape(TOKENS_PER_SHARD, QUERY_HEADS * HEAD_SIZE).astype(jnp.bfloat16)
    attended = lax.map(one_block, (block_list, orders)).reshape(NEW_TOKENS, QUERY_HEADS * HEAD_SIZE)
    return jnp.dot(attended, out_weight, preferred_element_type=jnp.float32).astype(jnp.bfloat16)
```

```python
import functools
import math

import jax
import jax.numpy as jnp
from jax import lax
from jax.experimental import pallas as pl
from jax.experimental.pallas import tpu as pltpu
from jax.sharding import PartitionSpec as P

QUERY_HEADS = 128
KEY_VALUE_HEADS = 8
HEAD_SIZE = 128
CACHE_DEV = 512

GROUP = QUERY_HEADS // KEY_VALUE_HEADS
ROW_BLOCK = 128
BLOCKS_PER_STEP = 4
HEADS_PER_STEP = 4
NEVER = 2**30
masked_floor = -1e30


def attention_kernel(last_block, steps_ref, table_ref, query_ref, own_ref, order_ref, kv_ref, out_ref):
    tokens = query_ref.shape[0]
    heads = query_ref.shape[1] // HEAD_SIZE
    queries = jnp.concatenate(
        [query_ref[:, h * HEAD_SIZE : (h + 1) * HEAD_SIZE] for h in range(heads)], axis=0
    )
    factor = math.log2(math.e) / math.sqrt(HEAD_SIZE)
    own = jnp.concatenate([own_ref[...]] * heads, axis=1)

    def step(i, carry):
        peak, total, weighted = carry
        keys, values, orders = [], [], []
        for b in range(BLOCKS_PER_STEP):
            entry = table_ref[i * BLOCKS_PER_STEP + b]
            rows = pl.ds(pl.multiple_of(jnp.minimum(entry, last_block) * ROW_BLOCK, ROW_BLOCK), ROW_BLOCK)
            keys.append(kv_ref[0, rows, :])
            values.append(kv_ref[1, rows, :])
            marks = pl.ds(pl.multiple_of(entry * ROW_BLOCK, ROW_BLOCK), ROW_BLOCK)
            orders.append(order_ref[marks, :])
        scores = lax.dot_general(
            jnp.concatenate(keys, axis=0),
            queries,
            (((1,), (1,)), ((), ())),
            preferred_element_type=jnp.float32,
        )
        order = jnp.concatenate(orders, axis=0)
        order = jnp.concatenate([order] * (tokens * heads // order.shape[1]), axis=1)
        scores = jnp.where(order <= own, scores, -jnp.inf)
        new_peak = jnp.maximum(peak, jnp.max(scores, axis=0, keepdims=True))
        rescale = jnp.exp2((peak - new_peak) * factor)
        raised = jnp.exp2((scores - new_peak) * factor)
        total = total * rescale + jnp.sum(raised, axis=0, keepdims=True)
        update = lax.dot_general(
            jnp.concatenate(values, axis=0),
            raised.astype(jnp.bfloat16),
            (((0,), (0,)), ((), ())),
            preferred_element_type=jnp.float32,
        )
        return new_peak, total, weighted * rescale + update

    width = tokens * heads
    start = (
        jnp.full((1, width), masked_floor, jnp.float32),
        jnp.zeros((1, width), jnp.float32),
        jnp.zeros((HEAD_SIZE, width), jnp.float32),
    )
    _, total, weighted = lax.fori_loop(0, steps_ref[0], step, start)
    result = weighted / total
    for h in range(heads):
        out_ref[:, h * HEAD_SIZE : (h + 1) * HEAD_SIZE] = result[:, h * tokens : (h + 1) * tokens].T.astype(
            out_ref.dtype
        )


def attention(queries, kv_all, own_order, order_all, lengths_all):
    tokens, columns = queries.shape
    kv_rows = kv_all.shape[1]
    shards = lengths_all.shape[0]
    shard_rows = kv_rows // shards
    kv_heads = kv_all.shape[2] // HEAD_SIZE
    per_group = GROUP // HEADS_PER_STEP
    slot = jnp.arange(CACHE_DEV)
    cache_order = jnp.where(slot[None, :] < lengths_all[:, None], -1, NEVER)
    row_order = jnp.concatenate([cache_order, order_all.reshape(shards, -1)], axis=1).reshape(kv_rows)
    row_order = jnp.concatenate([row_order, jnp.full((ROW_BLOCK,), NEVER, jnp.int32)])
    row_order = jnp.broadcast_to(row_order[:, None], (kv_rows + ROW_BLOCK, 128)).astype(jnp.int32)
    blocks = kv_rows // ROW_BLOCK
    within = jnp.arange(shard_rows // ROW_BLOCK) * ROW_BLOCK
    wanted = ((within[None, :] >= CACHE_DEV) | (within[None, :] < lengths_all[:, None])).reshape(blocks)
    place = jnp.cumsum(wanted.astype(jnp.int32)) - 1
    slots = -(-blocks // BLOCKS_PER_STEP) * BLOCKS_PER_STEP
    hit = wanted[None, :] & (place[None, :] == jnp.arange(slots)[:, None])
    table = jnp.where(
        jnp.any(hit, axis=1), jnp.sum(jnp.where(hit, jnp.arange(blocks)[None, :], 0), axis=1), blocks
    ).astype(jnp.int32)
    count = jnp.sum(wanted.astype(jnp.int32))
    steps = ((count + BLOCKS_PER_STEP - 1) // BLOCKS_PER_STEP).reshape(1).astype(jnp.int32)
    query_block = HEADS_PER_STEP * HEAD_SIZE
    return pl.pallas_call(
        functools.partial(attention_kernel, blocks - 1),
        out_shape=jax.ShapeDtypeStruct((tokens, columns), jnp.bfloat16),
        grid_spec=pltpu.PrefetchScalarGridSpec(
            num_scalar_prefetch=2,
            grid=(kv_heads, per_group),
            in_specs=[
                pl.BlockSpec((tokens, query_block), lambda g, h, *_: (0, g * per_group + h)),
                pl.BlockSpec((1, tokens), lambda g, h, *_: (0, 0)),
                pl.BlockSpec((kv_rows + ROW_BLOCK, 128), lambda g, h, *_: (0, 0)),
                pl.BlockSpec((2, kv_rows, HEAD_SIZE), lambda g, h, *_: (0, 0, g)),
            ],
            out_specs=pl.BlockSpec((tokens, query_block), lambda g, h, *_: (0, g * per_group + h)),
        ),
        compiler_params=pltpu.CompilerParams(vmem_limit_bytes=40 * 1024 * 1024),
        cost_estimate=pl.CostEstimate(
            flops=4 * tokens * columns * kv_rows, bytes_accessed=8 * 2**20, transcendentals=tokens * kv_rows * 32
        ),
        name="attend",
    )(steps, table, queries, own_order[None, :], row_order, kv_all)


def gather_metadata(cache_lengths, token_order):
    tokens = token_order.shape[0]
    packed = lax.all_gather(jnp.concatenate([token_order, cache_lengths]), "ctx", axis=0, tiled=False)
    return packed[:, :tokens].reshape(-1), packed[:, tokens]


def body(queries, key_value_cache, cache_lengths, token_order, out_weight):
    order_all, lengths_all = gather_metadata(cache_lengths, token_order)
    kv_all = lax.all_gather(key_value_cache, "ctx", axis=1, tiled=True)
    attended = attention(queries, kv_all, token_order, order_all, lengths_all)
    terms = jnp.dot(
        lax.all_gather(attended, "ctx", axis=0, tiled=True),
        out_weight,
        preferred_element_type=jnp.float32,
    )
    return lax.psum_scatter(terms.astype(jnp.bfloat16), "tp", scatter_dimension=0, tiled=True)


def solution(mesh):
    placed = (P("ctx", "tp"), P(None, "ctx", "tp"), P("ctx"), P("ctx"), P("tp", "ctx"))
    return jax.shard_map(
        body, mesh=mesh, in_specs=placed, out_specs=P("tp", "ctx"), check_vma=False
    )
```

```python
import functools
import math

import jax
import jax.numpy as jnp
from jax import lax
from jax.experimental import pallas as pl
from jax.experimental.pallas import tpu as pltpu
from jax.sharding import PartitionSpec as P

QUERY_HEADS = 128
KEY_VALUE_HEADS = 8
HEAD_SIZE = 128
CACHE_DEV = 512

GROUP = QUERY_HEADS // KEY_VALUE_HEADS
ROW_BLOCK = 128
BLOCKS_PER_STEP = 4
HEADS_PER_STEP = 8
PIECES = 2
NEVER = 2**30
masked_floor = -1e30


def attention_kernel(last_block, steps_ref, table_ref, query_ref, own_ref, order_ref, kv_ref, out_ref):
    tokens = query_ref.shape[0]
    heads = query_ref.shape[1] // HEAD_SIZE
    queries = jnp.concatenate(
        [query_ref[:, h * HEAD_SIZE : (h + 1) * HEAD_SIZE] for h in range(heads)], axis=0
    )
    factor = math.log2(math.e) / math.sqrt(HEAD_SIZE)
    own = own_ref[...]

    def step(i, carry):
        peak, total, weighted = carry
        keys, values, orders = [], [], []
        for b in range(BLOCKS_PER_STEP):
            entry = table_ref[i * BLOCKS_PER_STEP + b]
            rows = pl.ds(pl.multiple_of(jnp.minimum(entry, last_block) * ROW_BLOCK, ROW_BLOCK), ROW_BLOCK)
            keys.append(kv_ref[0, rows, :])
            values.append(kv_ref[1, rows, :])
            marks = pl.ds(pl.multiple_of(entry * ROW_BLOCK, ROW_BLOCK), ROW_BLOCK)
            orders.append(order_ref[marks, :])
        scores = lax.dot_general(
            jnp.concatenate(keys, axis=0),
            queries,
            (((1,), (1,)), ((), ())),
            preferred_element_type=jnp.float32,
        )
        order = jnp.concatenate(orders, axis=0)
        order = jnp.concatenate([order] * (tokens * heads // order.shape[1]), axis=1)
        scores = jnp.where(order <= own, scores, -jnp.inf)
        new_peak = jnp.maximum(peak, jnp.max(scores, axis=0, keepdims=True))
        rescale = jnp.exp2((peak - new_peak) * factor)
        raised = jnp.exp2((scores - new_peak) * factor)
        total = total * rescale + jnp.sum(raised, axis=0, keepdims=True)
        update = lax.dot_general(
            jnp.concatenate(values, axis=0),
            raised.astype(jnp.bfloat16),
            (((0,), (0,)), ((), ())),
            preferred_element_type=jnp.float32,
        )
        return new_peak, total, weighted * rescale + update

    width = tokens * heads
    start = (
        jnp.full((1, width), masked_floor, jnp.float32),
        jnp.zeros((1, width), jnp.float32),
        jnp.zeros((HEAD_SIZE, width), jnp.float32),
    )
    _, total, weighted = lax.fori_loop(0, steps_ref[0], step, start)
    result = (weighted / total).T
    for h in range(heads):
        out_ref[:, h * HEAD_SIZE : (h + 1) * HEAD_SIZE] = result[h * tokens : (h + 1) * tokens].astype(out_ref.dtype)


def attention_tables(kv_all, order_all, lengths_all):
    kv_rows = kv_all.shape[1]
    shards = lengths_all.shape[0]
    shard_rows = kv_rows // shards
    slot = jnp.arange(CACHE_DEV)
    cache_order = jnp.where(slot[None, :] < lengths_all[:, None], -1, NEVER)
    row_order = jnp.concatenate([cache_order, order_all.reshape(shards, -1)], axis=1).reshape(kv_rows)
    row_order = jnp.concatenate([row_order, jnp.full((ROW_BLOCK,), NEVER, jnp.int32)])
    row_order = jnp.broadcast_to(row_order[:, None], (kv_rows + ROW_BLOCK, 128)).astype(jnp.int32)
    blocks = kv_rows // ROW_BLOCK
    within = jnp.arange(shard_rows // ROW_BLOCK) * ROW_BLOCK
    wanted = ((within[None, :] >= CACHE_DEV) | (within[None, :] < lengths_all[:, None])).reshape(blocks)
    place = jnp.cumsum(wanted.astype(jnp.int32)) - 1
    slots = -(-blocks // BLOCKS_PER_STEP) * BLOCKS_PER_STEP
    hit = wanted[None, :] & (place[None, :] == jnp.arange(slots)[:, None])
    table = jnp.where(
        jnp.any(hit, axis=1), jnp.sum(jnp.where(hit, jnp.arange(blocks)[None, :], 0), axis=1), blocks
    ).astype(jnp.int32)
    count = jnp.sum(wanted.astype(jnp.int32))
    steps = ((count + BLOCKS_PER_STEP - 1) // BLOCKS_PER_STEP).reshape(1).astype(jnp.int32)
    return steps, table, row_order


def attention(queries, kv_all, own_order, steps, table, row_order):
    tokens, columns = queries.shape
    kv_rows = kv_all.shape[1]
    blocks = kv_rows // ROW_BLOCK
    kv_heads = kv_all.shape[2] // HEAD_SIZE
    per_group = GROUP // HEADS_PER_STEP
    query_block = HEADS_PER_STEP * HEAD_SIZE
    return pl.pallas_call(
        functools.partial(attention_kernel, blocks - 1),
        out_shape=jax.ShapeDtypeStruct((tokens, columns), jnp.bfloat16),
        grid_spec=pltpu.PrefetchScalarGridSpec(
            num_scalar_prefetch=2,
            grid=(kv_heads, per_group),
            in_specs=[
                pl.BlockSpec((tokens, query_block), lambda g, h, *_: (0, g * per_group + h)),
                pl.BlockSpec((1, tokens * HEADS_PER_STEP), lambda g, h, *_: (0, 0)),
                pl.BlockSpec((kv_rows + ROW_BLOCK, 128), lambda g, h, *_: (0, 0)),
                pl.BlockSpec((2, kv_rows, HEAD_SIZE), lambda g, h, *_: (0, 0, g)),
            ],
            out_specs=pl.BlockSpec((tokens, query_block), lambda g, h, *_: (0, g * per_group + h)),
        ),
        compiler_params=pltpu.CompilerParams(vmem_limit_bytes=40 * 1024 * 1024),
        cost_estimate=pl.CostEstimate(
            flops=4 * tokens * columns * kv_rows, bytes_accessed=8 * 2**20, transcendentals=tokens * kv_rows * 32
        ),
        name="attend",
    )(steps, table, queries, jnp.tile(own_order, HEADS_PER_STEP)[None, :], row_order, kv_all)


def gather_metadata(cache_lengths, token_order):
    tokens = token_order.shape[0]
    packed = lax.all_gather(jnp.concatenate([token_order, cache_lengths]), "ctx", axis=0, tiled=False)
    return packed[:, :tokens].reshape(-1), packed[:, tokens]


def body(queries, key_value_cache, cache_lengths, token_order, out_weight):
    order_all, lengths_all = gather_metadata(cache_lengths, token_order)
    kv_all = lax.all_gather(key_value_cache, "ctx", axis=1, tiled=True)
    tables = attention_tables(kv_all, order_all, lengths_all)
    tokens = queries.shape[0]
    piece = tokens // PIECES
    parts = []
    for number in range(PIECES):
        own = slice(number * piece, (number + 1) * piece)
        attended = attention(queries[own], kv_all, token_order[own], *tables)
        terms = jnp.dot(
            lax.all_gather(attended, "ctx", axis=0, tiled=True),
            out_weight,
            preferred_element_type=jnp.float32,
        )
        part = lax.psum_scatter(terms.astype(jnp.bfloat16), "tp", scatter_dimension=0, tiled=True)
        parts.append(part.reshape(-1, piece, part.shape[1]))
    return jnp.concatenate(parts, axis=1).reshape(-1, out_weight.shape[1])


def solution(mesh):
    placed = (P("ctx", "tp"), P(None, "ctx", "tp"), P("ctx"), P("ctx"), P("tp", "ctx"))
    return jax.shard_map(
        body, mesh=mesh, in_specs=placed, out_specs=P("tp", "ctx"), check_vma=False
    )
```
